32 devices in a mesh: dp: 1 (over z), tx: 4 (over y), ty: 8 (over x, core).
Axes of the slice: x: 4, y: 4, z: 1, core: 2. Of those that a mesh axis runs over, the one named last changes fastest.
The devices are a block of a 4x4x8 slice.
Arguments:
- residual: float32 [1024, 1536], P('dp', 'tx')
- norm_w: float32 [2, 1536], P(None, 'tx')
- w_in: bfloat16 [2, 1536, 2, 3072], P(None, 'tx', None, 'ty')
- conv_w: float32 [2, 3072, 4], P(None, 'ty')
- conv_b: float32 [2, 3072], P(None, 'ty')
- w_x: bfloat16 [2, 3072, 128], P(None, 'ty')
- w_dt: bfloat16 [2, 96, 3072], P(None, None, 'ty')
- dt_bias: float32 [2, 3072], P(None, 'ty')
- a_log: float32 [2, 3072, 16], P(None, 'ty')
- d_skip: float32 [2, 3072], P(None, 'ty')
- w_out: bfloat16 [2, 3072, 1536], P(None, 'ty', 'tx')
- conv_state: bfloat16 [2, 1024, 3072, 3], P(None, ('dp', 'tx'), 'ty')
- ssm_state: float32 [2, 1024, 3072, 16], P(None, ('dp', 'tx'), 'ty')
Outputs:
- output 1: float32 [1024, 1536], P('dp', 'tx')
- output 2: bfloat16 [2, 1024, 3072, 3], P(None, ('dp', 'tx'), 'ty')
- output 3: float32 [2, 1024, 3072, 16], P(None, ('dp', 'tx'), 'ty')
All inputs are finite; a program needn't handle non-finite values.
Results may differ from the reference program's by a relative error of at most 0.0169579.
Values are sent between devices in bfloat16 or wider.
A program may use at most 768 MiB of HBM per device.

```python
import math
import jax
import jax.numpy as jnp
from jax import lax

BATCH_ROWS = 1024
D_MODEL = 1536
D_INNER = 3072
D_STATE = 16
DT_RANK = 96
CONV_WIDTH = 4
LAYERS = 2
NORM_EPS = 1e-5
INNER_EPS = 1e-6


def setup_inputs(seed: int = 0, part: int = 0) -> dict:
    keys = jax.random.split(jax.random.key(seed), 10)
    row_keys = jax.random.split(jax.random.fold_in(jax.random.key(seed + 1), part), 3)
    col_pos = jnp.arange(D_MODEL, dtype=jnp.float32) / D_MODEL
    col_scale = jnp.exp(3.0 * col_pos - 1.5)
    residual = jax.random.normal(row_keys[0], (BATCH_ROWS, D_MODEL), jnp.float32) * col_scale
    norm_w = jax.random.uniform(keys[0], (LAYERS, D_MODEL), jnp.float32, 0.5, 1.5)
    w_in = (jax.random.normal(keys[1], (LAYERS, D_MODEL, 2, D_INNER), jnp.float32) * D_MODEL ** -0.5).astype(jnp.bfloat16)
    conv_w = jax.random.normal(keys[2], (LAYERS, D_INNER, CONV_WIDTH), jnp.float32) * CONV_WIDTH ** -0.5
    conv_b = jax.random.normal(keys[3], (LAYERS, D_INNER), jnp.float32) * 0.2
    w_x = (jax.random.normal(keys[4], (LAYERS, D_INNER, DT_RANK + 2 * D_STATE), jnp.float32) * D_INNER ** -0.5).astype(jnp.bfloat16)
    w_dt = (jax.random.normal(keys[5], (LAYERS, DT_RANK, D_INNER), jnp.float32) * DT_RANK ** -0.5).astype(jnp.bfloat16)
    dt_init = jnp.exp(jax.random.uniform(keys[6], (LAYERS, D_INNER), jnp.float32, math.log(0.005), math.log(0.1)))
    dt_bias = dt_init + jnp.log(-jnp.expm1(-dt_init))
    a_log = jnp.log(jax.random.uniform(keys[7], (LAYERS, D_INNER, D_STATE), jnp.float32, 1.0, 16.0))
    d_skip = jax.random.uniform(keys[8], (LAYERS, D_INNER), jnp.float32, 0.5, 2.0)
    w_out = (jax.random.normal(keys[9], (LAYERS, D_INNER, D_MODEL), jnp.float32) * D_INNER ** -0.5).astype(jnp.bfloat16)
    conv_state = jax.random.normal(row_keys[1], (LAYERS, BATCH_ROWS, D_INNER, CONV_WIDTH - 1), jnp.float32).astype(jnp.bfloat16)
    ssm_state = jax.random.normal(row_keys[2], (LAYERS, BATCH_ROWS, D_INNER, D_STATE), jnp.float32) * 0.5
    return {"residual": residual, "norm_w": norm_w, "w_in": w_in, "conv_w": conv_w, "conv_b": conv_b, "w_x": w_x, "w_dt": w_dt, "dt_bias": dt_bias, "a_log": a_log, "d_skip": d_skip, "w_out": w_out, "conv_state": conv_state, "ssm_state": ssm_state}


def unit_rms(vec):
    return vec * lax.rsqrt(jnp.mean(vec * vec, axis=-1, keepdims=True) + INNER_EPS)


def mixer_layer(residual, params):
    norm_w, w_in, conv_w, conv_b, w_x, w_dt, dt_bias, a_log, d_skip, w_out, conv_prev, ssm_prev = params
    variance = jnp.mean(residual * residual, axis=-1, keepdims=True)
    normed = (residual * lax.rsqrt(variance + NORM_EPS) * norm_w).astype(jnp.bfloat16)
    proj_in = jnp.dot(normed, w_in.reshape(D_MODEL, 2 * D_INNER), preferred_element_type=jnp.float32).astype(jnp.bfloat16)
    x_branch = proj_in[:, :D_INNER]
    z_branch = proj_in[:, D_INNER:]
    window = jnp.concatenate([conv_prev, x_branch[:, :, None]], axis=-1)
    conv_val = jnp.sum(window.astype(jnp.float32) * conv_w, axis=-1) + conv_b
    x_conv = jax.nn.silu(conv_val).astype(jnp.bfloat16)
    x_dbl = jnp.dot(x_conv, w_x, preferred_element_type=jnp.float32)
    dt_low = unit_rms(x_dbl[:, :DT_RANK])
    b_mat = unit_rms(x_dbl[:, DT_RANK:DT_RANK + D_STATE])
    c_mat = unit_rms(x_dbl[:, DT_RANK + D_STATE:])
    delta = jax.nn.softplus(jnp.dot(dt_low.astype(jnp.bfloat16), w_dt, preferred_element_type=jnp.float32) + dt_bias)
    x_float = x_conv.astype(jnp.float32)
    decay = jnp.exp(delta[:, :, None] * -jnp.exp(a_log))
    ssm_new = decay * ssm_prev + (delta * x_float)[:, :, None] * b_mat[:, None, :]
    state_val = jnp.sum(ssm_new * c_mat[:, None, :], axis=-1)
    gated = ((state_val + d_skip * x_float) * jax.nn.silu(z_branch.astype(jnp.float32))).astype(jnp.bfloat16)
    out_proj = jnp.dot(gated, w_out, preferred_element_type=jnp.float32)
    return residual + out_proj, (window[:, :, 1:], ssm_new)


def reference(residual, norm_w, w_in, conv_w, conv_b, w_x, w_dt, dt_bias, a_log, d_skip, w_out, conv_state, ssm_state):
    layer_params = (norm_w, w_in, conv_w, conv_b, w_x, w_dt, dt_bias, a_log, d_skip, w_out, conv_state, ssm_state)
    residual_out, caches = lax.scan(mixer_layer, residual, layer_params)
    return residual_out, caches[0], caches[1]
```

```python
import functools

import jax
import jax.numpy as jnp
from jax import lax
from jax.experimental import pallas as pl
from jax.experimental.pallas import tpu as pltpu
from jax.sharding import PartitionSpec as P

NORM_EPS = 1e-5
INNER_EPS = 1e-6
MESH = pl.DeviceIdType.MESH
F32 = jnp.float32
BF16 = jnp.bfloat16


def silu(v):
    return v * jax.nn.sigmoid(v)


def softplus(v):
    return jnp.maximum(v, 0.0) + jnp.log1p(jnp.exp(-jnp.abs(v)))


def loop(n, body):
    def step(i, carry):
        body(i)
        return carry

    lax.fori_loop(0, n, step, 0)


def mixer_kernel(names, nt, nj, n_state, *refs):
    R = dict(zip(names, refs))
    r0, nw, conv_w, conv_b = R["r0"], R["nw"], R["conv_w"], R["conv_b"]
    dt_bias, d_skip, a_log = R["dt_bias"], R["d_skip"], R["a_log"]
    rows_all, dm = r0.shape
    ch = a_log.shape[-1]
    rt = rows_all // nt
    half = rt // 2
    rj = rt // nj
    n_rank = R["px"].shape[-1] - 2 * n_state
    d_model = dm * nt

    t = lax.axis_index("tx")
    j = lax.axis_index("ty")
    tr, to, tl = lax.rem(t + 1, nt), lax.rem(t + 2, nt), lax.rem(t + 3, nt)
    core = lax.rem(j, 2)
    jp = j + 1 - 2 * core
    jr, jo, jl = lax.rem(j + 2, nj), lax.rem(j + 4, nj), lax.rem(j + 6, nj)
    x, xr, xo, xl = j // 2, jr // 2, jo // 2, jl // 2

    count = {"r": 0, "l": 0}
    sent = []

    def send(src, dst, **dev):
        i = count["r"]
        count["r"] += 1
        cp = pltpu.make_async_remote_copy(
            src_ref=src, dst_ref=dst, send_sem=R["send_sem"].at[i], recv_sem=R["recv_sem"].at[i],
            device_id=dev, device_id_type=MESH)
        cp.start()
        sent.append(cp)
        return cp

    def local(src, dst):
        i = count["l"]
        count["l"] += 1
        cp = pltpu.make_async_copy(src, dst, R["loc_sem"].at[i])
        cp.start()
        return cp

    ld_win0 = local(R["w_in"].at[0], R["w0"])
    ld_conv = local(R["conv_state"], R["convs"])
    ld_wx = local(R["w_x"], R["wx"])
    ld_wdt = local(R["w_dt"], R["wdt"])
    ld_wo = [local(R["w_out"].at[l], R["wo_g"].at[l, t]) for l in range(2)]
    ld_wi1 = [local(R["w_in"].at[1, k], R["wi_g"].at[k, t]) for k in range(2)]
    ld_ssm = [local(R["ssm"].at[l], R["st"].at[l]) for l in range(2)]

    barrier = pltpu.get_barrier_semaphore()
    for peer in (tr, to, tl):
        pl.semaphore_signal(barrier, inc=1, device_id={"tx": peer}, device_id_type=MESH)
    for peer in (jp, jr, jo, jl):
        pl.semaphore_signal(barrier, inc=1, device_id={"ty": peer}, device_id_type=MESH)

    def stat_body(b):
        rows = pl.ds(pl.multiple_of(b * 128, 128), 128)
        r = r0[rows, :]
        sq = r * r
        part = sq[:, :128]
        for i in range(1, dm // 128):
            part = part + sq[:, i * 128:(i + 1) * 128]
        R["stat"][pl.ds(b, 1), :] = jnp.sum(part.T, axis=0, keepdims=True)
        col = jnp.sum(part, axis=1, keepdims=True)
        lr = lax.rsqrt(col / dm + NORM_EPS)
        R["h0"][rows, :] = (r * lr * nw[0:1, :]).astype(BF16)

    loop(rows_all // 128, stat_body)
    pl.semaphore_wait(barrier, 7)
    stats = [send(R["stat"], R["stat_rx"].at[i], tx=p) for i, p in enumerate((tr, to, tl))]

    ld_win0.wait()
    pf, stg = R["pf"], R["stg"]

    def mm_body(b):
        rows = pl.ds(pl.multiple_of(b * 128, 128), 128)
        for k in range(2):
            pf[k, rows, :] = jnp.dot(R["h0"][rows, :], R["w0"][k], preferred_element_type=F32)

    loop(rows_all // 128, mm_body)
    for s in stats:
        s.wait_recv()

    def fac_body(b):
        rows = pl.ds(pl.multiple_of(b * 128, 128), 128)
        own = R["stat"][pl.ds(b, 1), :]
        tot = own
        for i in range(nt - 1):
            tot = tot + R["stat_rx"][i, pl.ds(b, 1), :]
        f = lax.rsqrt(tot / d_model + NORM_EPS) * jnp.sqrt(own / dm + NORM_EPS)
        fac = jnp.broadcast_to(f, (128, 128)).T
        R["fac"][rows, :] = fac
        for i in range(ch // 128):
            cols = slice(i * 128, (i + 1) * 128)
            v = pf[0, rows, cols] * fac
            pf[0, rows, cols] = v
            stg[0, rows, cols] = v.astype(BF16)

    loop(rows_all // 128, fac_body)
    rx, tx2 = R["rx"], R["tx2"]

    def part_rows(owner, h):
        return pl.ds(pl.multiple_of(owner * rt + h * half, half), half)

    def rs_first(k):
        return (send(stg.at[k, part_rows(to, 0)], rx.at[k, 0], tx=tr),
                send(stg.at[k, part_rows(to, 1)], rx.at[k, 1], tx=tl),
                send(stg.at[k, part_rows(tl, 0)], rx.at[k, 2], tx=tl),
                send(stg.at[k, part_rows(tr, 1)], rx.at[k, 3], tx=tr))

    def rs_second(k, first):
        first[0].wait_recv()
        tx2[k, 0] = (rx[k, 0].astype(F32) + pf[k, part_rows(tr, 0), :]).astype(BF16)
        a = send(tx2.at[k, 0], rx.at[k, 4], tx=tr)
        first[1].wait_recv()
        tx2[k, 1] = (rx[k, 1].astype(F32) + pf[k, part_rows(tl, 1), :]).astype(BF16)
        b = send(tx2.at[k, 1], rx.at[k, 5], tx=tl)
        return a, b

    def rs_last(k, first, second, out):
        for cp in (first[2], first[3], *second):
            cp.wait_recv()
        for h in range(2):
            v = pf[k, part_rows(t, h), :] + rx[k, 2 + h].astype(F32) + rx[k, 4 + h].astype(F32)
            out[h * half:(h + 1) * half, :] = v.astype(BF16)

    x_first = rs_first(0)

    def z_body(b):
        rows = pl.ds(pl.multiple_of(b * 128, 128), 128)
        fac = R["fac"][rows, :]
        for i in range(ch // 128):
            cols = slice(i * 128, (i + 1) * 128)
            v = pf[1, rows, cols] * fac
            pf[1, rows, cols] = v
            stg[1, rows, cols] = v.astype(BF16)

    loop(rows_all // 128, z_body)
    x_second = rs_second(0, x_first)
    z_first = rs_first(1)
    nw1 = R["nw1_g"]
    nw1[t] = nw[1:2, :]
    nw_cp = [send(nw1.at[t], nw1.at[t], tx=p) for p in (tr, to, tl)]
    r0g = R["r0g"]
    r0_cp = []
    for p in (tr, to, tl):
        src = r0.at[pl.ds(pl.multiple_of(p * rt + j * rj, rj), rj)]
        r0_cp.append(send(src, r0g.at[t], tx=p))
    r0g[t] = r0[pl.ds(pl.multiple_of(t * rt + j * rj, rj), rj), :]

    class Gather:
        def __init__(self, buf):
            self.buf, self.half = buf, buf.shape[1] // 2

        def own(self):
            self.a = send(self.buf.at[t], self.buf.at[t], tx=tr)
            self.b = send(self.buf.at[t], self.buf.at[t], tx=tl)

        def relay(self):
            self.a.wait_recv()
            lo, hi = pl.ds(0, self.half), pl.ds(self.half, self.half)
            self.c = send(self.buf.at[tl, lo], self.buf.at[tl, lo], tx=tr)
            self.b.wait_recv()
            self.d = send(self.buf.at[tr, hi], self.buf.at[tr, hi], tx=tl)

        def done(self):
            self.c.wait_recv()
            self.d.wait_recv()

    wo = [Gather(R["wo_g"].at[l]) for l in range(2)]
    wi = [Gather(R["wi_g"].at[k]) for k in range(2)]
    xib, zb, xcf, xcb = R["xib"], R["zb"], R["xcf"], R["xcb"]
    outs = []

    def conv_proj(l):
        def body(b):
            rows = pl.ds(pl.multiple_of(b * 32, 32), 32)
            v = xib[l, rows, :].astype(F32) * conv_w[l, 3:4, :]
            for i in range(3):
                v = v + R["convs"][l, i, rows, :].astype(F32) * conv_w[l, i:i + 1, :]
            xc = silu(v + conv_b[l:l + 1, :]).astype(BF16)
            xcb[l, rows, :] = xc
            xcf[rows, :] = xc.astype(F32)

        loop(rt // 32, body)
        p = jnp.dot(xcb[l], R["wx"][l], preferred_element_type=F32)
        R["px"][...] = p
        R["pst"][l] = p.astype(BF16)
        outs.append(local(xib.at[l], R["xi_out"].at[l]))
        outs.append(local(xcb.at[l], R["xc_out"].at[l]))

    def half_rows(c):
        return pl.ds(pl.multiple_of(c * half, half), half)

    def p_pair(l):
        return send(R["pst"].at[l, half_rows(1 - core)], R["pr0"].at[l], ty=jp)

    def p_cross(l, cp):
        cp.wait_recv()
        q = R["px"][half_rows(core), :] + R["pr0"][l].astype(F32)
        R["px"][half_rows(core), :] = q
        R["qs"][l] = q.astype(BF16)
        return [send(R["qs"].at[l], R["pr1"].at[l, i], ty=p) for i, p in enumerate((jr, jo, jl))]

    def p_finish(l, cps):
        for cp in cps:
            cp.wait_recv()
        q = R["px"][half_rows(core), :]
        for i in range(3):
            q = q + R["pr1"][l, i].astype(F32)
        R["px"][half_rows(core), :] = q
        R["tot"][l] = q.astype(BF16)
        cp = send(R["tot"].at[l], R["pr2"].at[l], ty=jp)
        cp.wait_recv()
        R["px"][half_rows(1 - core), :] = R["pr2"][l].astype(F32)

    def deltas(l):
        for h in range(2):
            rows = slice(h * half, (h + 1) * half)
            p = R["px"][rows, :]
            lane = lax.broadcasted_iota(jnp.int32, p.shape, 1)
            is_dt = lane < n_rank
            is_b = jnp.logical_and(lane >= n_rank, lane < n_rank + n_state)
            sq = p * p

            def scale_of(mask, n):
                tot = jnp.sum(jnp.where(mask, sq, 0.0), axis=1, keepdims=True)
                return lax.rsqrt(tot / n + INNER_EPS)

            s_dt = scale_of(is_dt, n_rank)
            s_b = scale_of(is_b, n_state)
            s_c = scale_of(lane >= n_rank + n_state, n_state)
            pn = p * jnp.where(is_dt, s_dt, jnp.where(is_b, s_b, s_c))
            low = jnp.where(is_dt, pn, 0.0).astype(BF16)
            raw = jnp.dot(low, R["wdt"][l], preferred_element_type=F32) + dt_bias[l:l + 1, :]
            R["dtb"][l, rows, :] = softplus(raw)
            bc = pn.T[n_rank:, :]
            for g in range(half // 8):
                R["btg"][l, h * (half // 8) + g] = pltpu.roll(bc, (half - 8 * g) % half, 1)
        outs.append(local(R["dtb"].at[l], R["dt_out"].at[l]))
        outs.append(local(R["btg"].at[l], R["bt_out"].at[l]))

    def scan_step(l):
        neg_a = -jnp.exp(a_log[l])
        skip = d_skip[l:l + 1, :]

        def body(g):
            rows = pl.ds(pl.multiple_of(g * 8, 8), 8)
            bt = R["btg"][l, g]
            dt8 = R["dtb"][l, rows, :]
            xc8 = xcf[rows, :]
            dx8 = dt8 * xc8
            ys = []
            for b in range(8):
                s = R["st"][l, g * 8 + b]
                b_col = jnp.broadcast_to(bt[:n_state, b:b + 1], s.shape)
                c_col = jnp.broadcast_to(bt[n_state:, b:b + 1], s.shape)
                s = jnp.exp(dt8[b:b + 1, :] * neg_a) * s + dx8[b:b + 1, :] * b_col
                ys.append(jnp.sum(s * c_col, axis=0, keepdims=True))
            R["ys"][rows, :] = jnp.concatenate(ys, axis=0) + skip * xc8

        loop(rt // 8, body)

    def gate():
        def body(b):
            rows = pl.ds(pl.multiple_of(b * 32, 32), 32)
            R["yb"][rows, :] = (R["ys"][rows, :] * silu(zb[rows, :].astype(F32))).astype(BF16)

        loop(rt // 32, body)

    of, ost, css, sums = R["of"], R["ost"], R["css"], R["sums"]

    def out_proj(l):
        for i in range(nt):
            o = jnp.dot(R["yb"][...], R["wo_g"][l, i], preferred_element_type=F32)
            for q in range(nj):
                v = o[q * rj:(q + 1) * rj, :]
                of[q, i] = v
                ost[l, q % 2, q // 2, i] = v.astype(BF16)
        return send(ost.at[l, 1 - core], R["opr"].at[l], ty=jp)

    def out_sums(l, cp):
        cp.wait_recv()

        def body(q):
            v = of[2 * q + core] + R["opr"][l, q].astype(F32)
            sums[q] = v
            css[l, q] = v.astype(BF16)

        loop(nj // 2, body)

    lo, hi = pl.ds(0, nt // 2), pl.ds(nt // 2, nt // 2)

    def out_reduce(l):
        ra, rb = R["rxs"], R["tx2s"]
        c0 = send(css.at[l, xo, lo], ra.at[l, 0], ty=jr)
        c1 = send(css.at[l, xo, hi], ra.at[l, 1], ty=jl)
        c2 = send(css.at[l, xl, lo], ra.at[l, 2], ty=jl)
        c3 = send(css.at[l, xr, hi], ra.at[l, 3], ty=jr)
        c0.wait_recv()
        rb[l, 0] = (ra[l, 0].astype(F32) + sums[xr, lo]).astype(BF16)
        c4 = send(rb.at[l, 0], ra.at[l, 4], ty=jr)
        c1.wait_recv()
        rb[l, 1] = (ra[l, 1].astype(F32) + sums[xl, hi]).astype(BF16)
        c5 = send(rb.at[l, 1], ra.at[l, 5], ty=jl)
        for cp in (c2, c3, c4, c5):
            cp.wait_recv()
        d = R["delta"]
        for h, part in enumerate((lo, hi)):
            v = sums[x, part] + ra[l, 2 + h].astype(F32) + ra[l, 4 + h].astype(F32)
            if l:
                v = v + d[part]
            d[part] = v

    def gather_ty(buf, between=None):
        a = send(buf.at[j], buf.at[j], ty=jr)
        b = send(buf.at[j], buf.at[j], ty=jl)
        waits = [send(buf.at[j], buf.at[j], ty=jp)]
        if between is not None:
            between()
        a.wait_recv()
        c = send(buf.at[jl, lo], buf.at[jl, lo], ty=jr)
        waits.append(send(buf.at[jl], buf.at[jl], ty=jp))
        b.wait_recv()
        d = send(buf.at[jr, hi], buf.at[jr, hi], ty=jl)
        waits.append(send(buf.at[jr], buf.at[jr], ty=jp))
        c.wait_recv()
        waits.append(send(buf.at[jo, lo], buf.at[jo, lo], ty=jp))
        d.wait_recv()
        waits.append(send(buf.at[jo, hi], buf.at[jo, hi], ty=jp))
        for cp in waits:
            cp.wait_recv()

    ld_conv.wait()
    ld_wx.wait()
    rs_last(0, x_first, x_second, xib.at[0])
    conv_proj(0)
    cp = p_pair(0)
    cps = p_cross(0, cp)
    z_second = rs_second(1, z_first)
    for cp in ld_wo:
        cp.wait()
    wo[0].own()
    ld_wdt.wait()
    p_finish(0, cps)
    deltas(0)
    ld_ssm[0].wait()
    scan_step(0)
    rs_last(1, z_first, z_second, zb)
    gate()
    for cp in ld_wi1:
        cp.wait()
    wo[0].relay()
    wi[0].own()
    wo[0].done()
    cp = out_proj(0)
    out_sums(0, cp)
    out_reduce(0)

    for cp in (*r0_cp, *nw_cp):
        cp.wait_recv()
    r1 = r0g[...] + R["delta"][...]
    ms = jnp.sum(jnp.sum(r1 * r1, axis=2, keepdims=True), axis=0, keepdims=True) / d_model
    hg = R["hg"]
    hg[j] = (r1 * lax.rsqrt(ms + NORM_EPS) * nw1[...]).astype(BF16)

    gather_ty(hg)
    wi[0].relay()
    wi[1].own()
    wi[0].done()

    def in_proj(k, out):
        acc = None
        for i in range(nt):
            d = jnp.dot(hg[:, i].reshape(rt, dm), R["wi_g"][k, i], preferred_element_type=F32)
            acc = d if acc is None else acc + d
        out[...] = acc.astype(BF16)

    in_proj(0, xib.at[1])
    conv_proj(1)
    cp = p_pair(1)
    cps = p_cross(1, cp)
    p_finish(1, cps)
    wi[1].relay()
    wo[1].own()
    deltas(1)
    ld_ssm[1].wait()
    scan_step(1)
    wi[1].done()
    in_proj(1, zb)
    gate()
    wo[1].relay()
    wo[1].done()
    cp = out_proj(1)
    out_sums(1, cp)
    out_reduce(1)

    fin, dst = R["fin"], R["dst"]
    dst[...] = R["delta"][...].astype(BF16)
    last = [send(dst.at[p], fin.at[j, t], tx=p) for p in (tr, to, tl)]
    fin[j, t] = dst[t]
    for cp in last:
        cp.wait_recv()
    gather_ty(fin)
    outs.append(local(fin, R["fin_out"]))

    for cp in outs:
        cp.wait()
    for cp in sent:
        cp.wait_send()


def state_kernel(n_state, ssm, dt, xc, bt, a_log, conv, xi, r0, fin, ssm_out, conv_out, r_out):
    neg_a = -jnp.exp(a_log[0])
    rows = dt.shape[1]
    for g in range(rows // 8):
        sl = slice(g * 8, (g + 1) * 8)
        b_all = bt[0, g]
        dt8 = dt[0, sl, :]
        dx8 = dt8 * xc[0, sl, :].astype(F32)
        for b in range(8):
            s = ssm[0, g * 8 + b]
            b_col = jnp.broadcast_to(b_all[:n_state, b:b + 1], s.shape)
            ssm_out[0, g * 8 + b] = jnp.exp(dt8[b:b + 1, :] * neg_a) * s + dx8[b:b + 1, :] * b_col
    conv_out[0, 0] = conv[0, 1]
    conv_out[0, 1] = conv[0, 2]
    conv_out[0, 2] = xi[0]
    rj = fin.shape[2]
    for q in range(fin.shape[0]):
        sl = slice(q * rj, (q + 1) * rj)
        r_out[sl, :] = r0[sl, :] + fin[q, 0].astype(F32)


def solution(mesh):
    nt, nj = mesh.shape["tx"], mesh.shape["ty"]

    def local_step(residual, norm_w, w_in, conv_w, conv_b, w_x, w_dt, dt_bias, a_log, d_skip, w_out, conv_state, ssm_state):
        n_l, rt, ch, n_state = ssm_state.shape
        rows_all, dm = residual.shape
        n_px = w_x.shape[-1]
        half, rj = rt // 2, rt // nj
        w_in_k = jnp.transpose(w_in, (0, 2, 1, 3))
        conv_w_t = jnp.transpose(conv_w, (0, 2, 1))
        a_log_t = jnp.transpose(a_log, (0, 2, 1))
        conv_t = jnp.transpose(conv_state, (0, 3, 1, 2))
        ssm_t = jnp.transpose(ssm_state, (0, 1, 3, 2))
        w_dt_p = jnp.pad(w_dt, ((0, 0), (0, n_px - w_dt.shape[1]), (0, 0)))

        vm = pl.BlockSpec(memory_space=pltpu.VMEM)
        hb = pl.BlockSpec(memory_space=pl.ANY)
        ins = [("r0", residual, vm), ("nw", norm_w, vm), ("conv_w", conv_w_t, vm), ("conv_b", conv_b, vm),
               ("dt_bias", dt_bias, vm), ("d_skip", d_skip, vm), ("a_log", a_log_t, vm),
               ("w_in", w_in_k, hb), ("w_x", w_x, hb), ("w_dt", w_dt_p, hb), ("w_out", w_out, hb),
               ("conv_state", conv_t, hb), ("ssm", ssm_t, hb)]
        S = jax.ShapeDtypeStruct
        outs = [("fin_out", S((nj, nt, rj, dm), BF16)), ("xi_out", S((n_l, rt, ch), BF16)), ("xc_out", S((n_l, rt, ch), BF16)),
                ("dt_out", S((n_l, rt, ch), F32)), ("bt_out", S((n_l, rt // 8, 2 * n_state, half), F32))]
        V = pltpu.VMEM
        scratch = [("w0", V((2, dm, ch), BF16)), ("convs", V((n_l, 3, rt, ch), BF16)), ("wx", V((n_l, ch, n_px), BF16)),
                   ("wdt", V((n_l, n_px, ch), BF16)), ("wo_g", V((n_l, nt, ch, dm), BF16)), ("wi_g", V((2, nt, dm, ch), BF16)),
                   ("st", V((n_l, rt, n_state, ch), F32)), ("stat", V((rows_all // 128, 128), F32)),
                   ("stat_rx", V((nt - 1, rows_all // 128, 128), F32)), ("h0", V((rows_all, dm), BF16)),
                   ("pf", V((2, rows_all, ch), F32)), ("stg", V((2, rows_all, ch), BF16)), ("fac", V((rows_all, 128), F32)),
                   ("rx", V((2, 6, half, ch), BF16)), ("tx2", V((2, 2, half, ch), BF16)),
                   ("nw1_g", V((nt, 1, dm), F32)), ("r0g", V((nt, rj, dm), F32)),
                   ("xib", V((n_l, rt, ch), BF16)), ("zb", V((rt, ch), BF16)), ("xcf", V((rt, ch), F32)), ("xcb", V((n_l, rt, ch), BF16)),
                   ("px", V((rt, n_px), F32)), ("pst", V((n_l, rt, n_px), BF16)), ("pr0", V((n_l, half, n_px), BF16)),
                   ("pr1", V((n_l, 3, half, n_px), BF16)), ("pr2", V((n_l, half, n_px), BF16)), ("qs", V((n_l, half, n_px), BF16)),
                   ("tot", V((n_l, half, n_px), BF16)), ("dtb", V((n_l, rt, ch), F32)),
                   ("btg", V((n_l, rt // 8, 2 * n_state, half), F32)), ("ys", V((rt, ch), F32)), ("yb", V((rt, ch), BF16)),
                   ("of", V((nj, nt, rj, dm), F32)), ("ost", V((n_l, 2, nj // 2, nt, rj, dm), BF16)),
                   ("opr", V((n_l, nj // 2, nt, rj, dm), BF16)), ("css", V((n_l, nj // 2, nt, rj, dm), BF16)),
                   ("sums", V((nj // 2, nt, rj, dm), F32)), ("rxs", V((n_l, 6, nt // 2, rj, dm), BF16)),
                   ("tx2s", V((n_l, 2, nt // 2, rj, dm), BF16)), ("delta", V((nt, rj, dm), F32)),
                   ("hg", V((nj, nt, rj, dm), BF16)), ("fin", V((nj, nt, rj, dm), BF16)), ("dst", V((nt, rj, dm), BF16)),
                   ("send_sem", pltpu.SemaphoreType.DMA((88,))), ("recv_sem", pltpu.SemaphoreType.DMA((88,))),
                   ("loc_sem", pltpu.SemaphoreType.DMA((24,)))]
        names = [n for n, *_ in ins] + [n for n, _ in outs] + [n for n, _ in scratch]
        fin, xi, xc, dt, bt = pl.pallas_call(
            functools.partial(mixer_kernel, names, nt, nj, n_state),
            out_shape=[s for _, s in outs],
            in_specs=[s for _, _, s in ins],
            out_specs=[hb] * len(outs),
            scratch_shapes=[s for _, s in scratch],
            compiler_params=pltpu.CompilerParams(collective_id=0, has_side_effects=True, vmem_limit_bytes=60 * 2**20),
            name="mixer",
        )(*[a for _, a, _ in ins])

        rb = 32
        n_b = rt // rb
        rr = rows_all // (n_l * n_b)
        qj = rr // rj
        per_t = rt // rr
        ssm_new, conv_new, r_new = pl.pallas_call(
            functools.partial(state_kernel, n_state),
            grid=(n_l, n_b),
            in_specs=[pl.BlockSpec((1, rb, n_state, ch), lambda l, b: (l, b, 0, 0)),
                      pl.BlockSpec((1, rb, ch), lambda l, b: (l, b, 0)),
                      pl.BlockSpec((1, rb, ch), lambda l, b: (l, b, 0)),
                      pl.BlockSpec((1, rb // 8, 2 * n_state, half), lambda l, b: (l, b, 0, 0)),
                      pl.BlockSpec((1, n_state, ch), lambda l, b: (l, 0, 0)),
                      pl.BlockSpec((1, 3, rb, ch), lambda l, b: (l, 0, b, 0)),
                      pl.BlockSpec((1, rb, ch), lambda l, b: (l, b, 0)),
                      pl.BlockSpec((rr, dm), lambda l, b: (l * n_b + b, 0)),
                      pl.BlockSpec((qj, 1, rj, dm), lambda l, b: (lax.rem(l * n_b + b, per_t), (l * n_b + b) // per_t, 0, 0))],
            out_specs=[pl.BlockSpec((1, rb, n_state, ch), lambda l, b: (l, b, 0, 0)),
                       pl.BlockSpec((1, 3, rb, ch), lambda l, b: (l, 0, b, 0)),
                       pl.BlockSpec((rr, dm), lambda l, b: (l * n_b + b, 0))],
            out_shape=[S(ssm_t.shape, F32), S(conv_t.shape, BF16), S((rows_all, dm), F32)],
            compiler_params=pltpu.CompilerParams(dimension_semantics=("arbitrary", "arbitrary")),
            name="state",
        )(ssm_t, dt, xc, bt, a_log_t, conv_t, xi, residual, fin)
        return r_new, jnp.transpose(conv_new, (0, 2, 3, 1)), jnp.transpose(ssm_new, (0, 1, 3, 2))

    cache_spec = P(None, ("dp", "tx"), "ty", None)
    in_specs = (P("dp", "tx"), P(None, "tx"), P(None, "tx", None, "ty"), P(None, "ty", None), P(None, "ty"), P(None, "ty", None), P(None, None, "ty"), P(None, "ty"), P(None, "ty", None), P(None, "ty"), P(None, "ty", "tx"), cache_spec, cache_spec)
    out_specs = (P("dp", "tx"), cache_spec, cache_spec)
    return jax.shard_map(local_step, mesh=mesh, in_specs=in_specs, out_specs=out_specs, check_vma=False)
```

```python
import functools

import jax
import jax.numpy as jnp
from jax import lax
from jax.experimental import pallas as pl
from jax.experimental.pallas import tpu as pltpu
from jax.sharding import PartitionSpec as P

NORM_EPS = 1e-5
INNER_EPS = 1e-6
LOG2E = 1.4426950408889634
MESH = pl.DeviceIdType.MESH
F32 = jnp.float32
BF16 = jnp.bfloat16


def silu(v):
    return v * jax.nn.sigmoid(v)


def softplus(v):
    return jnp.maximum(v, 0.0) + jnp.log1p(jnp.exp(-jnp.abs(v)))


def loop(n, body):
    def step(i, carry):
        body(i)
        return carry

    lax.fori_loop(0, n, step, 0)


def fold_rows(vs):
    row = lax.broadcasted_iota(jnp.int32, vs[0].shape, 0)
    k = 1
    while len(vs) > 1:
        low = (row & k) == 0
        vs = [jnp.where(low, a, b) + pltpu.roll(jnp.where(low, b, a), 8 - k, 0) for a, b in zip(vs[::2], vs[1::2])]
        k *= 2
    return vs[0]


def mixer_kernel(names, nt, nj, n_state, *refs):
    R = dict(zip(names, refs))
    r0, nw, conv_w, conv_b = R["r0v"], R["nwv"], R["conv_wv"], R["conv_bv"]
    dt_bias, d_skip, a_log = R["dt_biasv"], R["d_skipv"], R["a_logv"]
    rows_all, dm = r0.shape
    ch = a_log.shape[-1]
    rt = rows_all // nt
    half = rt // 2
    rj = rt // nj
    n_rank = R["px"].shape[-1] - 2 * n_state
    d_model = dm * nt

    t = lax.axis_index("tx")
    j = lax.axis_index("ty")
    tr, to, tl = lax.rem(t + 1, nt), lax.rem(t + 2, nt), lax.rem(t + 3, nt)
    core = lax.rem(j, 2)
    jp = j + 1 - 2 * core
    jr, jo, jl = lax.rem(j + 2, nj), lax.rem(j + 4, nj), lax.rem(j + 6, nj)
    x, xr, xo, xl = j // 2, jr // 2, jo // 2, jl // 2

    count = {"r": 0, "l": 0}
    sent = []

    def send(src, dst, **dev):
        i = count["r"]
        count["r"] += 1
        cp = pltpu.make_async_remote_copy(
            src_ref=src, dst_ref=dst, send_sem=R["send_sem"].at[i], recv_sem=R["recv_sem"].at[i],
            device_id=dev, device_id_type=MESH)
        cp.start()
        sent.append(cp)
        return cp

    def local(src, dst):
        i = count["l"]
        count["l"] += 1
        cp = pltpu.make_async_copy(src, dst, R["loc_sem"].at[i])
        cp.start()
        return cp

    barrier = pltpu.get_barrier_semaphore()
    for peer in (tr, to, tl):
        pl.semaphore_signal(barrier, inc=1, device_id={"tx": peer}, device_id_type=MESH)
    for peer in (jp, jr, jo, jl):
        pl.semaphore_signal(barrier, inc=1, device_id={"ty": peer}, device_id_type=MESH)

    ld_r0 = [local(R["r0"], r0), local(R["nw"], nw)]
    ld_win0 = local(R["w_in"].at[0], R["w0"])
    ld_small = [local(R[n], R[n + "v"]) for n in ("conv_w", "conv_b", "dt_bias", "d_skip", "a_log")]
    ld_conv = [local(R["conv_state"].at[l, 0], R["convs"].at[l]) for l in range(2)]
    ld_conv += [local(R["conv_state"].at[l, pl.ds(1, 2)], R["conv_out"].at[l, pl.ds(0, 2)]) for l in range(2)]
    ld_wx = local(R["w_x"], R["wx"])
    R["wdt"][:, n_rank:, :] = jnp.zeros_like(R["wdt"][:, n_rank:, :])
    ld_wdt = local(R["w_dt"], R["wdt"].at[:, pl.ds(0, n_rank)])
    ld_wo = [local(R["w_out"].at[l], R["wo_g"].at[l, t]) for l in range(2)]
    ld_wi1 = [local(R["w_in"].at[1, k], R["wi_g"].at[k, t]) for k in range(2)]
    ld_ssm = [local(R["ssm"].at[l], R["ssm_out"].at[l]) for l in range(2)]

    for cp in ld_r0:
        cp.wait()

    def stat_body(b):
        rows = pl.ds(pl.multiple_of(b * 128, 128), 128)
        r = r0[rows, :]
        sq = r * r
        part = sq[:, :128]
        for i in range(1, dm // 128):
            part = part + sq[:, i * 128:(i + 1) * 128]
        R["stat"][pl.ds(b, 1), :] = jnp.sum(part.T, axis=0, keepdims=True)
        col = jnp.sum(part, axis=1, keepdims=True)
        lr = lax.rsqrt(col / dm + NORM_EPS)
        R["h0"][rows, :] = (r * lr * nw[0:1, :]).astype(BF16)

    loop(rows_all // 128, stat_body)
    ld_win0.wait()
    pf, stg = R["pf"], R["stg"]

    def mm(k):
        def body(b):
            rows = pl.ds(pl.multiple_of(b * rt, rt), rt)
            v = jnp.dot(R["h0"][rows, :], R["w0"][k], preferred_element_type=F32)
            pf[k, rows, :] = v
            stg[k, rows, :] = v.astype(BF16)

        loop(nt, body)

    mm(0)
    rx, tx2 = R["rx"], R["tx2"]
    pl.semaphore_wait(barrier, 7)
    stats = [send(R["stat"], R["stat_rx"].at[i], tx=p) for i, p in enumerate((tr, to, tl))]

    def part_rows(owner, h):
        return pl.ds(pl.multiple_of(owner * rt + h * half, half), half)

    def rs_first(k):
        return (send(stg.at[k, part_rows(to, 0)], rx.at[k, 0], tx=tr),
                send(stg.at[k, part_rows(to, 1)], rx.at[k, 1], tx=tl),
                send(stg.at[k, part_rows(tl, 0)], rx.at[k, 2], tx=tl),
                send(stg.at[k, part_rows(tr, 1)], rx.at[k, 3], tx=tr))

    def factors():
        picks = ((0, 2 * tr), (None, 2 * tr), (2, 2 * tl + 1), (None, 2 * tl + 1), (None, 2 * t), (2, 2 * t), (None, 2 * t + 1), (0, 2 * t + 1))
        for i, (slot, blk) in enumerate(picks):
            own = R["stat"][pl.ds(blk, 1), :]
            tot = own
            for q in range(nt - 1):
                tot = tot + R["stat_rx"][q, pl.ds(blk, 1), :]
            src = own if slot is None else R["stat_rx"][slot, pl.ds(blk, 1), :]
            f = lax.rsqrt(tot / d_model + NORM_EPS) * jnp.sqrt(src / dm + NORM_EPS)
            R["fac"][i] = jnp.broadcast_to(f, (half, half)).T

    def scaled(v, i):
        return v.astype(F32) * jnp.concatenate([R["fac"][i]] * (ch // half), axis=1)

    def rs_second(k, first):
        first[0].wait_recv()
        tx2[k, 0] = (scaled(rx[k, 0], 0) + scaled(pf[k, part_rows(tr, 0), :], 1)).astype(BF16)
        a = send(tx2.at[k, 0], rx.at[k, 4], tx=tr)
        first[1].wait_recv()
        tx2[k, 1] = (scaled(rx[k, 1], 2) + scaled(pf[k, part_rows(tl, 1), :], 3)).astype(BF16)
        b = send(tx2.at[k, 1], rx.at[k, 5], tx=tl)
        return a, b

    def rs_last(k, first, second, out):
        for cp in (first[2], first[3], *second):
            cp.wait_recv()
        for h in range(2):
            v = scaled(pf[k, part_rows(t, h), :], 4 + 2 * h) + scaled(rx[k, 2 + h], 5 + 2 * h) + rx[k, 4 + h].astype(F32)
            out[h * half:(h + 1) * half, :] = v.astype(BF16)

    x_first = rs_first(0)
    mm(1)
    for cp in stats:
        cp.wait_recv()
    factors()
    x_second = rs_second(0, x_first)
    z_first = rs_first(1)

    class Gather:
        def __init__(self, buf):
            self.buf, self.half = buf, buf.shape[1] // 2

        def half_send(self, owner, hi, peer):
            part = self.buf.at[owner, pl.ds(hi * self.half, self.half)]
            return send(part, part, tx=peer)

        def own(self):
            self.a = [self.half_send(t, h, tr) for h in (0, 1)]
            self.b = [self.half_send(t, h, tl) for h in (1, 0)]

        def relay(self):
            self.a[0].wait_recv()
            self.c = self.half_send(tl, 0, tr)
            self.b[0].wait_recv()
            self.d = self.half_send(tr, 1, tl)

        def done(self):
            for cp in (self.a[1], self.b[1], self.c, self.d):
                cp.wait_recv()

    wo = [Gather(R["wo_g"].at[l]) for l in range(2)]
    wi = [Gather(R["wi_g"].at[k]) for k in range(2)]
    zb, xcf, xcb = R["zb"], R["xcf"], R["xcb"]
    caches = R["conv_out"]

    def conv_proj(l):
        def body(b):
            rows = pl.ds(pl.multiple_of(b * 32, 32), 32)
            v = R["convs"][l, rows, :].astype(F32) * conv_w[l, 0:1, :]
            for i in range(3):
                v = v + caches[l, i, rows, :].astype(F32) * conv_w[l, i + 1:i + 2, :]
            xc = silu(v + conv_b[l:l + 1, :]).astype(BF16)
            xcb[rows, :] = xc
            xcf[rows, :] = xc.astype(F32)

        loop(rt // 32, body)
        p = jnp.dot(xcb[...], R["wx"][l], preferred_element_type=F32)
        R["px"][...] = p
        R["pst"][l] = p.astype(BF16)

    def half_rows(c):
        return pl.ds(pl.multiple_of(c * half, half), half)

    def p_pair(l):
        return send(R["pst"].at[l, half_rows(1 - core)], R["pr0"].at[l], ty=jp)

    def p_cross(l, cp):
        cp.wait_recv()
        q = R["px"][half_rows(core), :] + R["pr0"][l].astype(F32)
        R["px"][half_rows(core), :] = q
        R["qs"][l] = q.astype(BF16)
        return [send(R["qs"].at[l], R["pr1"].at[l, i], ty=p) for i, p in enumerate((jr, jo, jl))]

    def p_scan(l, cps, between=None):
        for cp in cps:
            cp.wait_recv()
        q = R["px"][half_rows(core), :]
        for i in range(3):
            q = q + R["pr1"][l, i].astype(F32)
        R["px"][half_rows(core), :] = q
        R["tot"][l] = q.astype(BF16)
        cp = send(R["tot"].at[l], R["pr2"].at[l], ty=jp)
        deltas(l, core)
        scan_step(l, core)
        if between is not None:
            between()
        cp.wait_recv()
        R["px"][half_rows(1 - core), :] = R["pr2"][l].astype(F32)
        deltas(l, 1 - core)
        scan_step(l, 1 - core)

    def deltas(l, h):
        if True:
            rows = half_rows(h)
            p = R["px"][rows, :]
            lane = lax.broadcasted_iota(jnp.int32, p.shape, 1)
            is_dt = lane < n_rank
            is_b = jnp.logical_and(lane >= n_rank, lane < n_rank + n_state)
            sq = p * p

            def scale_of(mask, n):
                tot = jnp.sum(jnp.where(mask, sq, 0.0), axis=1, keepdims=True)
                return lax.rsqrt(tot / n + INNER_EPS)

            s_dt = scale_of(is_dt, n_rank)
            s_b = scale_of(is_b, n_state)
            s_c = scale_of(lane >= n_rank + n_state, n_state)
            pn = p * jnp.where(is_dt, s_dt, jnp.where(is_b, s_b, s_c))
            low = jnp.where(is_dt, pn, 0.0).astype(BF16)
            raw = jnp.dot(low, R["wdt"][l], preferred_element_type=F32) + dt_bias[l:l + 1, :]
            R["dtb"][rows, :] = softplus(raw)
            bc = pn.T[n_rank:, :]
            for g in range(half // 8):
                R["btg"][h * (half // 8) + g] = pltpu.roll(bc, (half - 8 * g) % half, 1)

    def scan_step(l, h):
        neg_a = -jnp.exp(a_log[l]) * LOG2E
        skip = d_skip[l:l + 1, :]

        def body(i):
            g = h * (half // 8) + i
            rows = pl.ds(pl.multiple_of(g * 8, 8), 8)
            bt = R["btg"][g]
            dt8 = R["dtb"][rows, :]
            xc8 = xcf[rows, :]
            dx8 = dt8 * xc8
            ys = []
            for b in range(8):
                s = R["ssm_out"][l, g * 8 + b]
                b_col = jnp.broadcast_to(bt[:n_state, b:b + 1], s.shape)
                c_col = jnp.broadcast_to(bt[n_state:, b:b + 1], s.shape)
                s = jnp.exp2(dt8[b:b + 1, :] * neg_a) * s + dx8[b:b + 1, :] * b_col
                R["ssm_out"][l, g * 8 + b] = s
                v = s * c_col
                ys.append(v[:8] + v[8:])
            R["ys"][rows, :] = fold_rows(ys) + skip * xc8

        loop(half // 8, body)

    def gate():
        def body(b):
            rows = pl.ds(pl.multiple_of(b * 32, 32), 32)
            R["yb"][rows, :] = (R["ys"][rows, :] * silu(zb[rows, :].astype(F32))).astype(BF16)

        loop(rt // 32, body)

    of, ost, css, sums = R["of"], R["ost"], R["css"], R["sums"]

    lo, hi = pl.ds(0, nt // 2), pl.ds(nt // 2, nt // 2)

    def out_reduce(l, between=None):
        pair = []
        for i in range(nt):
            o = jnp.dot(R["yb"][...], R["wo_g"][l, i], preferred_element_type=F32)
            for q in range(nj):
                v = o[q * rj:(q + 1) * rj, :]
                of[q, i] = v
                ost[l, q % 2, i, q // 2] = v.astype(BF16)
            pair.append(send(ost.at[l, 1 - core, i], R["opr"].at[l, i], ty=jp))
        ra, rb = R["rxs"], R["tx2s"]

        def chip_sum(i):
            pair[i].wait_recv()

            def body(q):
                v = of[2 * q + core, i] + R["opr"][l, i, q].astype(F32)
                sums[q, i] = v
                css[l, q, i] = v.astype(BF16)

            loop(nj // 2, body)

        chip_sum(0)
        chip_sum(1)
        c0 = send(css.at[l, xo, lo], ra.at[l, 0], ty=jr)
        c2 = send(css.at[l, xl, lo], ra.at[l, 2], ty=jl)
        chip_sum(2)
        chip_sum(3)
        c1 = send(css.at[l, xo, hi], ra.at[l, 1], ty=jl)
        c3 = send(css.at[l, xr, hi], ra.at[l, 3], ty=jr)
        c0.wait_recv()
        rb[l, 0] = (ra[l, 0].astype(F32) + sums[xr, lo]).astype(BF16)
        c4 = send(rb.at[l, 0], ra.at[l, 4], ty=jr)
        c1.wait_recv()
        rb[l, 1] = (ra[l, 1].astype(F32) + sums[xl, hi]).astype(BF16)
        c5 = send(rb.at[l, 1], ra.at[l, 5], ty=jl)
        if between is not None:
            between()
        for cp in (c2, c3, c4, c5):
            cp.wait_recv()
        d = R["delta"]
        for h, part in enumerate((lo, hi)):
            v = sums[x, part] + ra[l, 2 + h].astype(F32) + ra[l, 4 + h].astype(F32)
            if l:
                v = v + d[part]
            d[part] = v

    def gather_ty(buf, between=None):
        def part(owner, p, peer):
            return send(buf.at[owner, p], buf.at[owner, p], ty=peer)

        a = [part(j, p, jr) for p in (lo, hi)]
        b = [part(j, p, jl) for p in (hi, lo)]
        waits = [send(buf.at[j], buf.at[j], ty=jp)]
        a[0].wait_recv()
        c = part(jl, lo, jr)
        waits.append(part(jl, lo, jp))
        b[0].wait_recv()
        d = part(jr, hi, jl)
        waits.append(part(jr, hi, jp))
        a[1].wait_recv()
        waits.append(part(jl, hi, jp))
        b[1].wait_recv()
        waits.append(part(jr, lo, jp))
        if between is not None:
            between()
        c.wait_recv()
        waits.append(part(jo, lo, jp))
        d.wait_recv()
        waits.append(part(jo, hi, jp))
        for cp in waits:
            cp.wait_recv()

    for cp in (*ld_conv, ld_wx, *ld_small):
        cp.wait()
    rs_last(0, x_first, x_second, caches.at[0, 2])
    conv_proj(0)
    cp = p_pair(0)
    cps = p_cross(0, cp)
    z_second = rs_second(1, z_first)
    for cp in ld_wo:
        cp.wait()
    wo[0].own()
    nw1 = R["nw1_g"]
    nw1[t] = nw[1:2, :]
    nw_cp = [send(nw1.at[t], nw1.at[t], tx=p) for p in (tr, to, tl)]
    r0g = R["r0g"]
    r0_cp = []
    for p in (tr, to, tl):
        src = r0.at[pl.ds(pl.multiple_of(p * rt + j * rj, rj), rj)]
        r0_cp.append(send(src, r0g.at[t], tx=p))
    r0g[t] = r0[pl.ds(pl.multiple_of(t * rt + j * rj, rj), rj), :]
    ld_wdt.wait()
    ld_ssm[0].wait()
    p_scan(0, cps)
    rs_last(1, z_first, z_second, zb)
    gate()
    for cp in ld_wi1:
        cp.wait()
    wo[0].relay()
    wi[0].own()
    wo[0].done()
    def next_gate_weights():
        wi[0].relay()
        wi[1].own()

    out_reduce(0, next_gate_weights)

    for cp in (*r0_cp, *nw_cp):
        cp.wait_recv()
    r1 = r0g[...] + R["delta"][...]
    ms = jnp.sum(jnp.sum(r1 * r1, axis=2, keepdims=True), axis=0, keepdims=True) / d_model
    hg = R["hg"]
    hg[j] = (r1 * lax.rsqrt(ms + NORM_EPS) * nw1[...]).astype(BF16)

    def next_weights():
        wi[1].relay()
        wo[1].own()

    gather_ty(hg, next_weights)
    wi[0].done()

    def in_proj(k, out):
        acc = None
        for i in range(nt):
            d = jnp.dot(hg[:, i].reshape(rt, dm), R["wi_g"][k, i], preferred_element_type=F32)
            acc = d if acc is None else acc + d
        out[...] = acc.astype(BF16)

    in_proj(0, caches.at[1, 2])
    conv_proj(1)
    cp = p_pair(1)
    cps = p_cross(1, cp)
    ld_ssm[1].wait()
    p_scan(1, cps, wo[1].relay)
    wi[1].done()
    in_proj(1, zb)
    gate()
    wo[1].done()
    out_reduce(1)

    fin, dst = R["fin"], R["dst"]
    dst[...] = R["delta"][...].astype(BF16)
    last = [send(dst.at[p], fin.at[j, t], tx=p) for p in (tr, to, tl)]
    fin[j, t] = dst[t]
    for cp in last:
        cp.wait_recv()
    gather_ty(fin)

    def res_body(q):
        for i in range(nt):
            rows = pl.ds(pl.multiple_of(i * rt + q * rj, rj), rj)
            R["r_out"][rows, :] = r0[rows, :] + fin[q, i].astype(F32)

    loop(nj, res_body)
    for cp in sent:
        cp.wait_send()


def solution(mesh):
    nt, nj = mesh.shape["tx"], mesh.shape["ty"]

    def local_step(residual, norm_w, w_in, conv_w, conv_b, w_x, w_dt, dt_bias, a_log, d_skip, w_out, conv_state, ssm_state):
        n_l, rt, ch, n_state = ssm_state.shape
        rows_all, dm = residual.shape
        n_px = w_x.shape[-1]
        half, rj = rt // 2, rt // nj
        w_in_k = jnp.transpose(w_in, (0, 2, 1, 3))
        conv_w_t = jnp.transpose(conv_w, (0, 2, 1))
        a_log_t = jnp.transpose(a_log, (0, 2, 1))
        conv_t = jnp.transpose(conv_state, (0, 3, 1, 2))
        ssm_t = jnp.transpose(ssm_state, (0, 1, 3, 2))

        hb = pl.BlockSpec(memory_space=pl.ANY)
        ins = [("r0", residual, hb), ("nw", norm_w, hb), ("conv_w", conv_w_t, hb), ("conv_b", conv_b, hb),
               ("dt_bias", dt_bias, hb), ("d_skip", d_skip, hb), ("a_log", a_log_t, hb),
               ("w_in", w_in_k, hb), ("w_x", w_x, hb), ("w_dt", w_dt, hb), ("w_out", w_out, hb),
               ("conv_state", conv_t, hb), ("ssm", ssm_t, hb)]
        V = pltpu.VMEM
        outs = [("r_out", V(residual.shape, F32)), ("conv_out", V(conv_t.shape, BF16)), ("ssm_out", V(ssm_t.shape, F32))]
        scratch = [("r0v", V(residual.shape, F32)), ("nwv", V(norm_w.shape, F32)), ("conv_wv", V(conv_w_t.shape, F32)),
                   ("conv_bv", V(conv_b.shape, F32)), ("dt_biasv", V(dt_bias.shape, F32)), ("d_skipv", V(d_skip.shape, F32)),
                   ("a_logv", V(a_log_t.shape, F32)), ("w0", V((2, dm, ch), BF16)), ("convs", V((n_l, rt, ch), BF16)), ("wx", V((n_l, ch, n_px), BF16)),
                   ("wdt", V((n_l, n_px, ch), BF16)), ("wo_g", V((n_l, nt, ch, dm), BF16)), ("wi_g", V((2, nt, dm, ch), BF16)),
                   ("stat", V((rows_all // 128, 128), F32)),
                   ("stat_rx", V((nt - 1, rows_all // 128, 128), F32)), ("h0", V((rows_all, dm), BF16)),
                   ("pf", V((2, rows_all, ch), F32)), ("stg", V((2, rows_all, ch), BF16)), ("fac", V((8, half, half), F32)),
                   ("rx", V((2, 6, half, ch), BF16)), ("tx2", V((2, 2, half, ch), BF16)),
                   ("nw1_g", V((nt, 1, dm), F32)), ("r0g", V((nt, rj, dm), F32)),
                   ("zb", V((rt, ch), BF16)), ("xcf", V((rt, ch), F32)), ("xcb", V((rt, ch), BF16)),
                   ("px", V((rt, n_px), F32)), ("pst", V((n_l, rt, n_px), BF16)), ("pr0", V((n_l, half, n_px), BF16)),
                   ("pr1", V((n_l, 3, half, n_px), BF16)), ("pr2", V((n_l, half, n_px), BF16)), ("qs", V((n_l, half, n_px), BF16)),
                   ("tot", V((n_l, half, n_px), BF16)), ("dtb", V((rt, ch), F32)),
                   ("btg", V((rt // 8, 2 * n_state, half), F32)), ("ys", V((rt, ch), F32)), ("yb", V((rt, ch), BF16)),
                   ("of", V((nj, nt, rj, dm), F32)), ("ost", V((n_l, 2, nt, nj // 2, rj, dm), BF16)),
                   ("opr", V((n_l, nt, nj // 2, rj, dm), BF16)), ("css", V((n_l, nj // 2, nt, rj, dm), BF16)),
                   ("sums", V((nj // 2, nt, rj, dm), F32)), ("rxs", V((n_l, 6, nt // 2, rj, dm), BF16)),
                   ("tx2s", V((n_l, 2, nt // 2, rj, dm), BF16)), ("delta", V((nt, rj, dm), F32)),
                   ("hg", V((nj, nt, rj, dm), BF16)), ("fin", V((nj, nt, rj, dm), BF16)), ("dst", V((nt, rj, dm), BF16)),
                   ("send_sem", pltpu.SemaphoreType.DMA((120,))), ("recv_sem", pltpu.SemaphoreType.DMA((120,))),
                   ("loc_sem", pltpu.SemaphoreType.DMA((32,)))]
        names = [n for n, *_ in ins] + [n for n, _ in outs] + [n for n, _ in scratch]
        r_new, conv_new, ssm_new = pl.pallas_call(
            functools.partial(mixer_kernel, names, nt, nj, n_state),
            out_shape=[s for _, s in outs],
            in_specs=[s for _, _, s in ins],
            out_specs=[pl.BlockSpec(memory_space=V)] * len(outs),
            scratch_shapes=[s for _, s in scratch],
            compiler_params=pltpu.CompilerParams(collective_id=0, has_side_effects=True, vmem_limit_bytes=40 * 2**20),
            name="mixer",
        )(*[a for _, a, _ in ins])

        return r_new, jnp.transpose(conv_new, (0, 2, 3, 1)), jnp.transpose(ssm_new, (0, 1, 3, 2))

    cache_spec = P(None, ("dp", "tx"), "ty", None)
    in_specs = (P("dp", "tx"), P(None, "tx"), P(None, "tx", None, "ty"), P(None, "ty", None), P(None, "ty"), P(None, "ty", None), P(None, None, "ty"), P(None, "ty"), P(None, "ty", None), P(None, "ty"), P(None, "ty", "tx"), cache_spec, cache_spec)
    out_specs = (P("dp", "tx"), cache_spec, cache_spec)
    return jax.shard_map(local_step, mesh=mesh, in_specs=in_specs, out_specs=out_specs, check_vma=False)
```

```python
import functools
import math

import jax
import jax.numpy as jnp
from jax import lax
from jax.experimental import pallas as pl
from jax.experimental.pallas import tpu as pltpu
from jax.sharding import PartitionSpec as P

NORM_EPS = 1e-5
INNER_EPS = 1e-6
LOG2E = 1.4426950408889634
MESH = pl.DeviceIdType.MESH
F32 = jnp.float32
BF16 = jnp.bfloat16


def silu(v):
    return v * jax.nn.sigmoid(v)


def softplus(v):
    return jnp.maximum(v, 0.0) + jnp.log1p(jnp.exp(-jnp.abs(v)))


def loop(n, body):
    def step(i, carry):
        body(i)
        return carry

    lax.fori_loop(0, n, step, 0)


def fold_rows(vs):
    row = lax.broadcasted_iota(jnp.int32, vs[0].shape, 0)
    k = 1
    while len(vs) > 1:
        low = (row & k) == 0
        vs = [jnp.where(low, a, b) + pltpu.roll(jnp.where(low, b, a), 8 - k, 0) for a, b in zip(vs[::2], vs[1::2])]
        k *= 2
    return vs[0]


def mixer_kernel(names, nt, nj, n_state, *refs):
    R = dict(zip(names, refs))
    r0, nw, conv_w, conv_b = R["r0v"], R["nwv"], R["conv_wv"], R["conv_bv"]
    dt_bias, d_skip, a_log = R["dt_biasv"], R["d_skipv"], R["a_logv"]
    rows_all, dm = r0.shape
    ch = a_log.shape[-1]
    rt = rows_all // nt
    half = rt // 2
    rj = rt // nj
    n_rank = R["px"].shape[-1] - 2 * n_state
    d_model = dm * nt

    t = lax.axis_index("tx")
    j = lax.axis_index("ty")
    tr, to, tl = lax.rem(t + 1, nt), lax.rem(t + 2, nt), lax.rem(t + 3, nt)
    core = lax.rem(j, 2)
    jp = j + 1 - 2 * core
    jr, jo, jl = lax.rem(j + 2, nj), lax.rem(j + 4, nj), lax.rem(j + 6, nj)
    x, xr, xo, xl = j // 2, jr // 2, jo // 2, jl // 2

    count = {"r": 0, "l": 0, "s": 0, 0: 0, 1: 0, 2: 0}
    single = []
    drain = (R["ssm_out"].at[0], R["ssm_out"].at[0], R["btg"])
    unit = (n_state * ch * 4, n_state * ch * 4, 2 * n_state * half * 4)

    def send(src, dst, **dev):
        i = count["r"]
        count["r"] += 1
        size = math.prod(src.shape) * jnp.dtype(src.dtype).itemsize
        kind = next((k for k in range(3) if size % unit[k] == 0 and count[k] + size // unit[k] <= drain[k].shape[0]), None)
        if kind is None:
            sem = R["small_sem"].at[count["s"]]
            count["s"] += 1
        else:
            sem = R["send_sem"].at[kind]
            count[kind] += size // unit[kind]
        cp = pltpu.make_async_remote_copy(
            src_ref=src, dst_ref=dst, send_sem=sem, recv_sem=R["recv_sem"].at[i],
            device_id=dev, device_id_type=MESH)
        cp.start()
        if kind is None:
            single.append(cp)
        return cp

    def local(src, dst):
        i = count["l"]
        count["l"] += 1
        cp = pltpu.make_async_copy(src, dst, R["loc_sem"].at[i])
        cp.start()
        return cp

    barrier = pltpu.get_barrier_semaphore()
    for peer in (tr, to, tl):
        pl.semaphore_signal(barrier, inc=1, device_id={"tx": peer}, device_id_type=MESH)
    for peer in (jp, jr, jo, jl):
        pl.semaphore_signal(barrier, inc=1, device_id={"ty": peer}, device_id_type=MESH)

    ld_nw = local(R["nw"], nw)
    ld_r0 = [local(R["r0"].at[pl.ds(i * rt, rt)], r0.at[pl.ds(i * rt, rt)]) for i in range(nt)]
    ld_win = [local(R["w_in"].at[0], R["win"].at[0])]

    ld_nw.wait()

    def stat_body(b):
        rows = pl.ds(pl.multiple_of(b * 128, 128), 128)
        r = r0[rows, :]
        sq = r * r
        part = sq[:, :128]
        for i in range(1, dm // 128):
            part = part + sq[:, i * 128:(i + 1) * 128]
        R["stat"][pl.ds(b, 1), :] = jnp.sum(part.T, axis=0, keepdims=True)
        col = jnp.sum(part, axis=1, keepdims=True)
        lr = lax.rsqrt(col / dm + NORM_EPS)
        R["h0"][rows, :] = (r * lr * nw[0:1, :]).astype(BF16)

    def split_weights(l, k, out):
        def body(i):
            rows = pl.ds(pl.multiple_of(i * 32, 32), 32)
            out[rows, :] = R["win"][l, rows, k, :]

        loop(dm // 32, body)

    per = rt // 128
    for i in range(nt):
        ld_r0[i].wait()
        loop(per, lambda b, i=i: stat_body(i * per + b))
    ld_win.append(local(R["w_in"].at[1], R["win"].at[1]))
    ld_conv = [local(R["conv_state"].at[l, 0], R["convs"].at[l]) for l in range(2)]
    ld_conv += [local(R["conv_state"].at[l, pl.ds(1, 2)], R["conv_out"].at[l, pl.ds(0, 2)]) for l in range(2)]
    ld_small = [local(R[n], R[n + "v"]) for n in ("conv_w", "conv_b", "dt_bias", "d_skip", "a_log")]
    ld_wx = local(R["w_x"], R["wx"])
    ld_wdt = local(R["w_dt"], R["wdt"].at[:, pl.ds(0, n_rank)])
    ld_wo = [local(R["w_out"].at[l], R["wo_g"].at[l, t]) for l in range(2)]
    ld_ssm = [local(R["ssm"].at[l], R["ssm_out"].at[l]) for l in range(2)]
    ld_win[0].wait()
    split_weights(0, 0, R["w0"].at[0])
    pf, stg = R["pf"], R["stg"]

    def mm(k):
        def body(b):
            rows = pl.ds(pl.multiple_of(b * rt, rt), rt)
            v = jnp.dot(R["h0"][rows, :], R["w0"][k], preferred_element_type=F32)
            pf[k, rows, :] = v
            stg[k, rows, :] = v.astype(BF16)

        loop(nt, body)

    mm(0)
    rx, tx2 = R["rx"], R["tx2"]
    pl.semaphore_wait(barrier, 7)
    stats = [send(R["stat"], R["stat_rx"].at[i], tx=p) for i, p in enumerate((tr, to, tl))]

    def part_rows(owner, h):
        return pl.ds(pl.multiple_of(owner * rt + h * half, half), half)

    def rs_first(k):
        return (send(stg.at[k, part_rows(to, 0)], rx.at[k, 0], tx=tr),
                send(stg.at[k, part_rows(to, 1)], rx.at[k, 1], tx=tl),
                send(stg.at[k, part_rows(tl, 0)], rx.at[k, 2], tx=tl),
                send(stg.at[k, part_rows(tr, 1)], rx.at[k, 3], tx=tr))

    def factors():
        picks = ((0, 2 * tr), (None, 2 * tr), (2, 2 * tl + 1), (None, 2 * tl + 1), (None, 2 * t), (2, 2 * t), (None, 2 * t + 1), (0, 2 * t + 1))
        for i, (slot, blk) in enumerate(picks):
            own = R["stat"][pl.ds(blk, 1), :]
            tot = own
            for q in range(nt - 1):
                tot = tot + R["stat_rx"][q, pl.ds(blk, 1), :]
            src = own if slot is None else R["stat_rx"][slot, pl.ds(blk, 1), :]
            f = lax.rsqrt(tot / d_model + NORM_EPS) * jnp.sqrt(src / dm + NORM_EPS)
            R["fac"][i] = jnp.broadcast_to(f, (half, half)).T

    def scaled(v, i):
        return v.astype(F32) * jnp.concatenate([R["fac"][i]] * (ch // half), axis=1)

    def rs_second(k, first):
        first[0].wait_recv()
        tx2[k, 0] = (scaled(rx[k, 0], 0) + scaled(pf[k, part_rows(tr, 0), :], 1)).astype(BF16)
        a = send(tx2.at[k, 0], rx.at[k, 4], tx=tr)
        first[1].wait_recv()
        tx2[k, 1] = (scaled(rx[k, 1], 2) + scaled(pf[k, part_rows(tl, 1), :], 3)).astype(BF16)
        b = send(tx2.at[k, 1], rx.at[k, 5], tx=tl)
        return a, b

    def rs_last(k, first, second, out):
        for cp in (first[2], first[3], *second):
            cp.wait_recv()
        for h in range(2):
            v = scaled(pf[k, part_rows(t, h), :], 4 + 2 * h) + scaled(rx[k, 2 + h], 5 + 2 * h) + rx[k, 4 + h].astype(F32)
            out[h * half:(h + 1) * half, :] = v.astype(BF16)

    x_first = rs_first(0)
    split_weights(0, 1, R["w0"].at[1])
    mm(1)
    for cp in stats:
        cp.wait_recv()
    factors()
    x_second = rs_second(0, x_first)
    z_first = rs_first(1)
    R["wdt"][:, n_rank:, :] = jnp.zeros_like(R["wdt"][:, n_rank:, :])

    class Gather:
        def __init__(self, buf):
            self.buf, self.half = buf, buf.shape[1] // 2

        def half_send(self, owner, hi, peer):
            part = self.buf.at[owner, pl.ds(hi * self.half, self.half)]
            return send(part, part, tx=peer)

        def own(self):
            self.a = [self.half_send(t, h, tr) for h in (0, 1)]
            self.b = [self.half_send(t, h, tl) for h in (1, 0)]

        def relay(self):
            self.a[0].wait_recv()
            self.c = self.half_send(tl, 0, tr)
            self.b[0].wait_recv()
            self.d = self.half_send(tr, 1, tl)

        def done(self):
            for cp in (self.a[1], self.b[1], self.c, self.d):
                cp.wait_recv()

    wo = [Gather(R["wo_g"].at[l]) for l in range(2)]
    wi = [Gather(R["wi_g"].at[k]) for k in range(2)]
    zb, xcf, xcb = R["zb"], R["xcf"], R["xcb"]
    caches = R["conv_out"]

    def conv_proj(l):
        def body(b):
            rows = pl.ds(pl.multiple_of(b * 32, 32), 32)
            v = R["convs"][l, rows, :].astype(F32) * conv_w[l, 0:1, :]
            for i in range(3):
                v = v + caches[l, i, rows, :].astype(F32) * conv_w[l, i + 1:i + 2, :]
            xc = silu(v + conv_b[l:l + 1, :]).astype(BF16)
            xcb[rows, :] = xc
            xcf[rows, :] = xc.astype(F32)

        loop(rt // 32, body)
        p = jnp.dot(xcb[...], R["wx"][l], preferred_element_type=F32)
        R["px"][...] = p
        R["pst"][l] = p.astype(BF16)

    def half_rows(c):
        return pl.ds(pl.multiple_of(c * half, half), half)

    def p_pair(l):
        return send(R["pst"].at[l, half_rows(1 - core)], R["pr0"].at[l], ty=jp)

    def p_cross(l, cp):
        cp.wait_recv()
        q = R["px"][half_rows(core), :] + R["pr0"][l].astype(F32)
        R["px"][half_rows(core), :] = q
        R["qs"][l] = q.astype(BF16)
        return [send(R["qs"].at[l], R["pr1"].at[l, i], ty=p) for i, p in enumerate((jr, jo, jl))]

    def p_scan(l, cps, between=None):
        with jax.named_scope("P_cross_wait"):
            for cp in cps:
                cp.wait_recv()
        q = R["px"][half_rows(core), :]
        for i in range(3):
            q = q + R["pr1"][l, i].astype(F32)
        R["px"][half_rows(core), :] = q
        R["tot"][l] = q.astype(BF16)
        cp = send(R["tot"].at[l], R["pr2"].at[l], ty=jp)
        with jax.named_scope("P_deltas"):
            deltas(l, core)
        with jax.named_scope("P_scan"):
            scan_step(l, core)
        with jax.named_scope("P_between"):
            if between is not None:
                between()
        with jax.named_scope("P_pair_wait"):
            cp.wait_recv()
        R["px"][half_rows(1 - core), :] = R["pr2"][l].astype(F32)
        deltas(l, 1 - core)
        scan_step(l, 1 - core)

    def deltas(l, h):
        if True:
            rows = half_rows(h)
            p = R["px"][rows, :]
            lane = lax.broadcasted_iota(jnp.int32, p.shape, 1)
            is_dt = lane < n_rank
            is_b = jnp.logical_and(lane >= n_rank, lane < n_rank + n_state)
            sq = p * p

            def scale_of(mask, n):
                tot = jnp.sum(jnp.where(mask, sq, 0.0), axis=1, keepdims=True)
                return lax.rsqrt(tot / n + INNER_EPS)

            s_dt = scale_of(is_dt, n_rank)
            s_b = scale_of(is_b, n_state)
            s_c = scale_of(lane >= n_rank + n_state, n_state)
            pn = p * jnp.where(is_dt, s_dt, jnp.where(is_b, s_b, s_c))
            low = jnp.where(is_dt, pn, 0.0).astype(BF16)
            raw = jnp.dot(low, R["wdt"][l], preferred_element_type=F32) + dt_bias[l:l + 1, :]
            R["dtb"][rows, :] = softplus(raw)
            bc = pn.T[n_rank:, :]
            for g in range(half // 8):
                R["btg"][h * (half // 8) + g] = pltpu.roll(bc, (half - 8 * g) % half, 1)

    def scan_step(l, h):
        neg_a = -jnp.exp(a_log[l]) * LOG2E
        skip = d_skip[l:l + 1, :]

        def body(i):
            g = h * (half // 8) + i
            rows = pl.ds(pl.multiple_of(g * 8, 8), 8)
            bt = R["btg"][g]
            dt8 = R["dtb"][rows, :]
            xc8 = xcf[rows, :]
            dx8 = dt8 * xc8
            ys = []
            for b in range(8):
                s = R["ssm_out"][l, g * 8 + b]
                b_col = jnp.broadcast_to(bt[:n_state, b:b + 1], s.shape)
                c_col = jnp.broadcast_to(bt[n_state:, b:b + 1], s.shape)
                s = jnp.exp2(dt8[b:b + 1, :] * neg_a) * s + dx8[b:b + 1, :] * b_col
                R["ssm_out"][l, g * 8 + b] = s
                v = s * c_col
                ys.append(v[:8] + v[8:])
            R["ys"][rows, :] = fold_rows(ys) + skip * xc8

        loop(half // 8, body)

    def gate():
        def body(b):
            rows = pl.ds(pl.multiple_of(b * 32, 32), 32)
            R["yb"][rows, :] = (R["ys"][rows, :] * silu(zb[rows, :].astype(F32))).astype(BF16)

        loop(rt // 32, body)

    of, ost, css, sums = R["of"], R["ost"], R["css"], R["sums"]

    lo, hi = pl.ds(0, nt // 2), pl.ds(nt // 2, nt // 2)

    def out_reduce(l, between=None):
        pair = []
        for i in range(nt):
            o = jnp.dot(R["yb"][...], R["wo_g"][l, i], preferred_element_type=F32)
            for q in range(nj):
                v = o[q * rj:(q + 1) * rj, :]
                of[q, i] = v
                ost[l, q % 2, i, q // 2] = v.astype(BF16)
            pair.append(send(ost.at[l, 1 - core, i], R["opr"].at[l, i], ty=jp))
        ra, rb = R["rxs"], R["tx2s"]

        def chip_sum(i):
            pair[i].wait_recv()

            def body(q):
                v = of[2 * q + core, i] + R["opr"][l, i, q].astype(F32)
                sums[q, i] = v
                css[l, q, i] = v.astype(BF16)

            loop(nj // 2, body)

        chip_sum(0)
        chip_sum(1)
        c0 = send(css.at[l, xo, lo], ra.at[l, 0], ty=jr)
        c2 = send(css.at[l, xl, lo], ra.at[l, 2], ty=jl)
        chip_sum(2)
        chip_sum(3)
        c1 = send(css.at[l, xo, hi], ra.at[l, 1], ty=jl)
        c3 = send(css.at[l, xr, hi], ra.at[l, 3], ty=jr)
        c0.wait_recv()
        rb[l, 0] = (ra[l, 0].astype(F32) + sums[xr, lo]).astype(BF16)
        c4 = send(rb.at[l, 0], ra.at[l, 4], ty=jr)
        c1.wait_recv()
        rb[l, 1] = (ra[l, 1].astype(F32) + sums[xl, hi]).astype(BF16)
        c5 = send(rb.at[l, 1], ra.at[l, 5], ty=jl)
        if between is not None:
            between()
        for cp in (c2, c3, c4, c5):
            cp.wait_recv()
        d = R["delta"]
        for h, part in enumerate((lo, hi)):
            v = sums[x, part] + ra[l, 2 + h].astype(F32) + ra[l, 4 + h].astype(F32)
            if l:
                v = v + d[part]
            d[part] = v

    def gather_ty(buf, between=None):
        def part(owner, p, peer):
            return send(buf.at[owner, p], buf.at[owner, p], ty=peer)

        a = [part(j, p, jr) for p in (lo, hi)]
        b = [part(j, p, jl) for p in (hi, lo)]
        waits = [send(buf.at[j], buf.at[j], ty=jp)]
        a[0].wait_recv()
        c = part(jl, lo, jr)
        waits.append(part(jl, lo, jp))
        b[0].wait_recv()
        d = part(jr, hi, jl)
        waits.append(part(jr, hi, jp))
        a[1].wait_recv()
        waits.append(part(jl, hi, jp))
        b[1].wait_recv()
        waits.append(part(jr, lo, jp))
        if between is not None:
            between()
        c.wait_recv()
        waits.append(part(jo, lo, jp))
        d.wait_recv()
        waits.append(part(jo, hi, jp))
        for cp in waits:
            cp.wait_recv()

    for cp in (*ld_conv, ld_wx, *ld_small):
        cp.wait()
    rs_last(0, x_first, x_second, caches.at[0, 2])
    conv_proj(0)
    cp = p_pair(0)
    cps = p_cross(0, cp)
    z_second = rs_second(1, z_first)
    for cp in ld_wo:
        cp.wait()
    wo[0].own()
    ld_wdt.wait()
    ld_ssm[0].wait()
    p_scan(0, cps, wo[0].relay)
    rs_last(1, z_first, z_second, zb)
    gate()
    nw1 = R["nw1_g"]
    nw1[t] = nw[1:2, :]
    nw_cp = [send(nw1.at[t], nw1.at[t], tx=p) for p in (tr, to, tl)]
    r0g = R["r0g"]
    r0_cp = []
    for p in (tr, to, tl):
        src = r0.at[pl.ds(pl.multiple_of(p * rt + j * rj, rj), rj)]
        r0_cp.append(send(src, r0g.at[t], tx=p))
    r0g[t] = r0[pl.ds(pl.multiple_of(t * rt + j * rj, rj), rj), :]
    ld_win[1].wait()
    for k in range(2):
        split_weights(1, k, R["wi_g"].at[k, t])
    wi[0].own()
    wo[0].done()
    def next_gate_weights():
        wi[0].relay()
        wi[1].own()

    out_reduce(0, next_gate_weights)

    for cp in (*r0_cp, *nw_cp):
        cp.wait_recv()
    r1 = r0g[...] + R["delta"][...]
    ms = jnp.sum(jnp.sum(r1 * r1, axis=2, keepdims=True), axis=0, keepdims=True) / d_model
    hg = R["hg"]
    hg[j] = (r1 * lax.rsqrt(ms + NORM_EPS) * nw1[...]).astype(BF16)

    def next_weights():
        wi[1].relay()
        wo[1].own()

    gather_ty(hg, next_weights)
    wi[0].done()

    def in_proj(k, out):
        acc = None
        for i in range(nt):
            d = jnp.dot(hg[:, i].reshape(rt, dm), R["wi_g"][k, i], preferred_element_type=F32)
            acc = d if acc is None else acc + d
        out[...] = acc.astype(BF16)

    in_proj(0, caches.at[1, 2])
    conv_proj(1)
    cp = p_pair(1)
    cps = p_cross(1, cp)
    ld_ssm[1].wait()
    p_scan(1, cps, wo[1].relay)
    wi[1].done()
    in_proj(1, zb)
    gate()
    wo[1].done()
    out_reduce(1)

    fin, dst = R["fin"], R["dst"]
    dst[...] = R["delta"][...].astype(BF16)
    last = [send(dst.at[p], fin.at[j, t], tx=p) for p in (tr, to, tl)]
    fin[j, t] = dst[t]
    for cp in last:
        cp.wait_recv()
    gather_ty(fin)

    def res_body(q):
        for i in range(nt):
            rows = pl.ds(pl.multiple_of(i * rt + q * rj, rj), rj)
            R["r_out"][rows, :] = r0[rows, :] + fin[q, i].astype(F32)

    loop(nj, res_body)
    for cp in single:
        cp.wait_send()
    for k in range(3):
        taken = drain[k].at[pl.ds(0, count[k])]
        pltpu.make_async_copy(taken, taken, R["send_sem"].at[k]).wait()
    assert [count[c] for c in "rls"] == [R[n].shape[0] for n in ("recv_sem", "loc_sem", "small_sem")], count


def flush_kernel(*refs):
    n = (len(refs) - 1) // 2
    srcs, dsts, sem = refs[:n], refs[n:2 * n], refs[2 * n]
    cps = [pltpu.make_async_copy(s, d, sem.at[i]) for i, (s, d) in enumerate(zip(srcs, dsts))]
    for cp in cps:
        cp.start()
    for cp in cps:
        cp.wait()


def solution(mesh):
    nt, nj = mesh.shape["tx"], mesh.shape["ty"]

    def local_step(residual, norm_w, w_in, conv_w, conv_b, w_x, w_dt, dt_bias, a_log, d_skip, w_out, conv_state, ssm_state):
        n_l, rt, ch, n_state = ssm_state.shape
        rows_all, dm = residual.shape
        n_px = w_x.shape[-1]
        half, rj = rt // 2, rt // nj
        conv_w_t = jnp.transpose(conv_w, (0, 2, 1))
        a_log_t = jnp.transpose(a_log, (0, 2, 1))
        conv_t = jnp.transpose(conv_state, (0, 3, 1, 2))
        ssm_t = jnp.transpose(ssm_state, (0, 1, 3, 2))

        hb = pl.BlockSpec(memory_space=pl.ANY)
        ins = [("r0", residual, hb), ("nw", norm_w, hb), ("conv_w", conv_w_t, hb), ("conv_b", conv_b, hb),
               ("dt_bias", dt_bias, hb), ("d_skip", d_skip, hb), ("a_log", a_log_t, hb),
               ("w_in", w_in, hb), ("w_x", w_x, hb), ("w_dt", w_dt, hb), ("w_out", w_out, hb),
               ("conv_state", conv_t, hb), ("ssm", ssm_t, hb)]
        V = pltpu.VMEM
        outs = [("r_out", V(residual.shape, F32)), ("conv_out", V(conv_t.shape, BF16)), ("ssm_out", V(ssm_t.shape, F32))]
        scratch = [("r0v", V(residual.shape, F32)), ("nwv", V(norm_w.shape, F32)), ("conv_wv", V(conv_w_t.shape, F32)),
                   ("conv_bv", V(conv_b.shape, F32)), ("dt_biasv", V(dt_bias.shape, F32)), ("d_skipv", V(d_skip.shape, F32)),
                   ("a_logv", V(a_log_t.shape, F32)), ("win", V(w_in.shape, BF16)), ("w0", V((2, dm, ch), BF16)), ("convs", V((n_l, rt, ch), BF16)), ("wx", V((n_l, ch, n_px), BF16)),
                   ("wdt", V((n_l, n_px, ch), BF16)), ("wo_g", V((n_l, nt, ch, dm), BF16)), ("wi_g", V((2, nt, dm, ch), BF16)),
                   ("stat", V((rows_all // 128, 128), F32)),
                   ("stat_rx", V((nt - 1, rows_all // 128, 128), F32)), ("h0", V((rows_all, dm), BF16)),
                   ("pf", V((2, rows_all, ch), F32)), ("stg", V((2, rows_all, ch), BF16)), ("fac", V((8, half, half), F32)),
                   ("rx", V((2, 6, half, ch), BF16)), ("tx2", V((2, 2, half, ch), BF16)),
                   ("nw1_g", V((nt, 1, dm), F32)), ("r0g", V((nt, rj, dm), F32)),
                   ("zb", V((rt, ch), BF16)), ("xcf", V((rt, ch), F32)), ("xcb", V((rt, ch), BF16)),
                   ("px", V((rt, n_px), F32)), ("pst", V((n_l, rt, n_px), BF16)), ("pr0", V((n_l, half, n_px), BF16)),
                   ("pr1", V((n_l, 3, half, n_px), BF16)), ("pr2", V((n_l, half, n_px), BF16)), ("qs", V((n_l, half, n_px), BF16)),
                   ("tot", V((n_l, half, n_px), BF16)), ("dtb", V((rt, ch), F32)),
                   ("btg", V((rt // 8, 2 * n_state, half), F32)), ("ys", V((rt, ch), F32)), ("yb", V((rt, ch), BF16)),
                   ("of", V((nj, nt, rj, dm), F32)), ("ost", V((n_l, 2, nt, nj // 2, rj, dm), BF16)),
                   ("opr", V((n_l, nt, nj // 2, rj, dm), BF16)), ("css", V((n_l, nj // 2, nt, rj, dm), BF16)),
                   ("sums", V((nj // 2, nt, rj, dm), F32)), ("rxs", V((n_l, 6, nt // 2, rj, dm), BF16)),
                   ("tx2s", V((n_l, 2, nt // 2, rj, dm), BF16)), ("delta", V((nt, rj, dm), F32)),
                   ("hg", V((nj, nt, rj, dm), BF16)), ("fin", V((nj, nt, rj, dm), BF16)), ("dst", V((nt, rj, dm), BF16)),
                   ("send_sem", pltpu.SemaphoreType.DMA((3,))), ("small_sem", pltpu.SemaphoreType.DMA((6,))),
                   ("recv_sem", pltpu.SemaphoreType.DMA((104,))), ("loc_sem", pltpu.SemaphoreType.DMA((22,)))]
        names = [n for n, *_ in ins] + [n for n, _ in outs] + [n for n, _ in scratch]
        held = pl.pallas_call(
            functools.partial(mixer_kernel, names, nt, nj, n_state),
            out_shape=[s for _, s in outs],
            in_specs=[s for _, _, s in ins],
            out_specs=[pl.BlockSpec(memory_space=V)] * len(outs),
            scratch_shapes=[s for _, s in scratch],
            compiler_params=pltpu.CompilerParams(collective_id=0, has_side_effects=True, vmem_limit_bytes=40 * 2**20),
            name="mixer",
        )(*[a for _, a, _ in ins])

        r_new, conv_new, ssm_new = pl.pallas_call(
            flush_kernel,
            out_shape=[jax.ShapeDtypeStruct(a.shape, a.dtype) for a in held],
            in_specs=[pl.BlockSpec(memory_space=V)] * 3,
            out_specs=[hb] * 3,
            scratch_shapes=[pltpu.SemaphoreType.DMA((3,))],
            compiler_params=pltpu.CompilerParams(vmem_limit_bytes=2**20),
            name="flush",
        )(*[pltpu.with_memory_space_constraint(a, V) for a in held])
        return r_new, jnp.transpose(conv_new, (0, 2, 3, 1)), jnp.transpose(ssm_new, (0, 1, 3, 2))

    cache_spec = P(None, ("dp", "tx"), "ty", None)
    in_specs = (P("dp", "tx"), P(None, "tx"), P(None, "tx", None, "ty"), P(None, "ty", None), P(None, "ty"), P(None, "ty", None), P(None, None, "ty"), P(None, "ty"), P(None, "ty", None), P(None, "ty"), P(None, "ty", "tx"), cache_spec, cache_spec)
    out_specs = (P("dp", "tx"), cache_spec, cache_spec)
    return jax.shard_map(local_step, mesh=mesh, in_specs=in_specs, out_specs=out_specs, check_vma=False)
```
